32 devices in a mesh: tm: 8 (over z, x), space: 4 (over y, core).
Axes of the slice: x: 2, y: 2, z: 4, core: 2. Of those that a mesh axis runs over, the one named last changes fastest.
Arguments:
- state: float32 [32, 16, 64, 128], P('tm', 'space'), may hold values from -6 to 6
- source: float32 [32, 16, 64, 128], P('tm', 'space'), may hold values from -6 to 6
- absorption: float32 [16, 64, 128], P('space'), may hold values from 0.05 to 0.5
Outputs:
- relaxed: float32 [32, 16, 64, 128], P('tm', 'space')
- coarse_residual: float32 [8, 16, 64, 128], P('tm', 'space')
- residual_norm: float32 [], replicated
The draws below stay inside these ranges and needn't reach their ends.
All inputs are finite; a program needn't handle non-finite values.
Results may differ from the reference program's by a relative error of at most 0.0004.
Values sent between devices are 32-bit elements; how exact they have to be, the bound alone decides.
No kernel may reach another device: no remote copies, remote signals or barrier semaphores. Data moves between devices by JAX's collectives and lax.ppermute only.
A program may use at most 64 MiB of HBM per device.

```python
import math
import jax
import jax.numpy as jnp

NX = 64
NY = 128
CF = 4
SWEEPS = 5
NC = 8
NT = 32
NZ = 16


def shard_levels(stream_key, dims, cuts, low, high):
    level, own = 1.0, jax.random.fold_in(stream_key, 6)
    for dim, shards_of in cuts:
        steps = jnp.exp(jax.random.uniform(jax.random.fold_in(own, dim), (shards_of,), jnp.float32, low / len(cuts), high / len(cuts)))
        level = level * jnp.repeat(steps, dims[dim] // shards_of).reshape([-1 if axis == dim else 1 for axis in range(len(dims))])
    return level


def scatter_about(key, dims, deviation, limit, split=(), kind=jnp.bfloat16):
    drawn = deviation * jax.random.normal(key, dims, jnp.float32)
    if split:
        drawn = drawn * shard_levels(key, dims, split, -0.22, 0.18)
    return jnp.clip(drawn, -limit, limit).astype(kind)


def setup_inputs(seed: int = 0) -> dict:
    arg_keys = jax.random.split(jax.random.key(seed), 4)
    return {
        "state": scatter_about(arg_keys[0], (NT, NZ, NX, NY), 1.0, 6.0, ((0, 8), (1, 4)), jnp.float32),
        "source": scatter_about(arg_keys[1], (NT, NZ, NX, NY), 1.0, 6.0, ((0, 8), (1, 4)), jnp.float32),
        "absorption": jnp.clip(jnp.exp(math.log(0.5) - 2.3025851 * jax.random.uniform(arg_keys[2], (NZ, NX, NY), jnp.float32) ** shard_levels(arg_keys[2], (NZ, NX, NY), ((0, 4),), -0.2, 0.2)), 0.05, 0.5),
    }


coupling = 4.0


def sweep_weights(count):
    spread = 6.0 * coupling / (1.0 + 6.0 * coupling)
    return [1.0 / (1.0 + spread * math.cos(math.pi * (2 * k + 1) / (2 * count))) for k in range(count)]


def apply_operator(field, diag):
    lead = [(0, 0)] * (field.ndim - 3)
    padded = jnp.pad(field, lead + [(1, 1), (1, 1), (1, 1)])
    beside = padded[..., 2:, 1:-1, 1:-1] + padded[..., :-2, 1:-1, 1:-1]
    beside = beside + padded[..., 1:-1, 2:, 1:-1] + padded[..., 1:-1, :-2, 1:-1]
    beside = beside + padded[..., 1:-1, 1:-1, 2:] + padded[..., 1:-1, 1:-1, :-2]
    return diag * field - coupling * beside


def implicit_step(rhs, diag):
    field = rhs / diag
    for weight in sweep_weights(SWEEPS):
        field = field + weight * (rhs - apply_operator(field, diag)) / diag
    return field


def reference(state, source, absorption):
    diag = 1.0 + 6.0 * coupling + absorption
    fine = state.reshape(NC, CF, NZ, NX, NY)
    rhs = source.reshape(NC, CF, NZ, NX, NY)
    points = [fine[:, j] for j in range(CF)]

    def relax_fine(points):
        for j in range(1, CF):
            points[j] = implicit_step(points[j - 1], diag) + rhs[:, j]
        return points

    def previous(last):
        return jnp.concatenate([jnp.zeros_like(last[:1]), last[:-1]], axis=0)

    points = relax_fine(points)
    points[0] = implicit_step(previous(points[-1]), diag) + rhs[:, 0]
    points = relax_fine(points)
    coarse_residual = rhs[:, 0] + implicit_step(previous(points[-1]), diag) - points[0]
    relaxed = jnp.stack(points, axis=1).reshape(NT, NZ, NX, NY)
    return relaxed, coarse_residual, jnp.sum(coarse_residual * coarse_residual)
```

```python
import functools
import math

import jax
import jax.numpy as jnp
from jax import lax
from jax.experimental import pallas as pl
from jax.experimental.pallas import tpu as pltpu
from jax.sharding import PartitionSpec as P

SWEEPS = 5
COUPLING = 4.0
ROWS = 8


def sweep_weights(count):
    spread = 6.0 * COUPLING / (1.0 + 6.0 * COUPLING)
    return [
        1.0 / (1.0 + spread * math.cos(math.pi * (2 * k + 1) / (2 * count))) for k in range(count)
    ]


def step_polynomial():
    rest = [0.0, 1.0]
    for w in sweep_weights(SWEEPS):
        grown = [0.0] * (len(rest) + 1)
        for i, c in enumerate(rest):
            grown[i] += c * (1.0 - w)
            grown[i + 1] += c * w
        rest = grown
    top = [-c for c in rest]
    top[0] += 1.0
    quotient, carry = [], 0.0
    for c in top[:-1]:
        carry += c
        quotient.append(carry)
    return quotient[0], quotient[2], quotient[4]


def partner(value, axis, bit):
    count = lax.axis_size(axis)
    return lax.ppermute(value, axis, [(i, i ^ bit) for i in range(count)])


def next_slab(value):
    count = lax.axis_size("tm")
    return lax.ppermute(value, "tm", [(i, i + 1) for i in range(count - 1)])


def pieces_of(value):
    count = lax.axis_size("space")
    blocks = [value]
    bit = count // 2
    found = {0: value}
    while bit:
        found.update({m ^ bit: partner(v, "space", bit) for m, v in list(found.items())})
        bit //= 2
    return [found[m] for m in range(count)]


def chain_kernel(count, steps, keep, idx_ref, *refs):
    first = refs[:count]
    rest = refs[count : 2 * count]
    refs = refs[2 * count :]
    if keep:
        before_ref, relaxed_ref, change_ref, norm_ref = refs[:4]
        refs = refs[4:]
    else:
        last_ref, whole_ref = refs[:2]
        refs = refs[2:]
    h_ref, g_ref, a_ref, b_ref, c_ref, d_ref, s_ref, u_ref = refs
    planes, groups, rows, lanes = g_ref.shape
    depth = first[0].shape[-3]
    idx = idx_ref[0]
    c0, c1, c2 = (c / COUPLING for c in step_polynomial())

    def strided(k):
        return pl.ds(k, rows, stride=groups)

    for m in range(count):
        base = (idx ^ m) * depth
        for z in range(depth):
            for k in range(groups):
                diag = 1.0 + 6.0 * COUPLING + rest[m][steps - 1, z, strided(k), :]
                h = COUPLING / diag
                h_ref[base + z, k] = h
                g_ref[base + z, k] = h * first[m][z, strided(k), :]
                for j in range(steps - 1):
                    s_ref[j, base + z, k] = rest[m][j, z, strided(k), :]
                s_ref[steps - 1, base + z, k] = jnp.zeros((rows, lanes), jnp.float32)

    row = lax.broadcasted_iota(jnp.int32, (rows, lanes), 0)
    lane = lax.broadcasted_iota(jnp.int32, (rows, lanes), 1)
    not_top, not_bottom = row != 0, row != rows - 1
    not_left, not_right = lane != 0, lane != lanes - 1

    def jacobi(f_ref, z):
        field = [f_ref[z, k] for k in range(groups)]
        above = jnp.where(not_top, pltpu.roll(field[-1], 1, 0), 0.0)
        below = jnp.where(not_bottom, pltpu.roll(field[0], rows - 1, 0), 0.0)
        for k in range(groups):
            total = (field[k - 1] if k else above) + (field[k + 1] if k < groups - 1 else below)
            if z:
                total = total + f_ref[z - 1, k]
            if z < planes - 1:
                total = total + f_ref[z + 1, k]
            left = jnp.where(not_left, pltpu.roll(field[k], 1, 1), 0.0)
            right = jnp.where(not_right, pltpu.roll(field[k], lanes - 1, 1), 0.0)
            yield k, h_ref[z, k] * (total + (left + right))

    def step(j, carry):
        def level0(z):
            for k, v in jacobi(g_ref, z):
                a_ref[z, k] = v

        def level1(z):
            for k, v in jacobi(a_ref, z):
                b_ref[z, k] = c1 * g_ref[z, k] + c2 * v

        def level2(z):
            for k, v in jacobi(b_ref, z):
                c_ref[z, k] = v

        def level3(z):
            for k, v in jacobi(c_ref, z):
                d_ref[z, k] = c0 * g_ref[z, k] + v

        def level4(z):
            for k, v in jacobi(d_ref, z):
                u = (d_ref[z, k] + v) + s_ref[j, z, k]
                u_ref[j, z, k] = u
                g_ref[z, k] = h_ref[z, k] * u

        levels = [level0, level1, level2, level3, level4]
        for t in range(planes + 2 * (len(levels) - 1)):
            for i, level in enumerate(levels):
                z = t - 2 * i
                if 0 <= z < planes:
                    level(z)
        return carry

    lax.fori_loop(0, steps, step, 0)

    own = idx * depth
    if keep:
        partial = [jnp.zeros((rows, lanes), jnp.float32)] * groups
        for z in range(planes):
            for k in range(groups):
                change = u_ref[steps - 1, z, k] - before_ref[z, k]
                a_ref[z, k] = change
                partial[k] = partial[k] + change * change
        for z in range(depth):
            for k in range(groups):
                at = strided(k)
                relaxed_ref[0, z, at, :] = first[0][z, at, :]
                for j in range(steps - 1):
                    relaxed_ref[j + 1, z, at, :] = u_ref[j, own + z, k]
                change_ref[z, at, :] = a_ref[own + z, k]
        partial = jnp.sum(functools.reduce(jnp.add, partial), axis=0, keepdims=True)
        total = jnp.sum(partial, axis=1, keepdims=True) * idx_ref[1].astype(jnp.float32)
        norm_ref[...] = jnp.broadcast_to(total, norm_ref.shape)
    else:
        for z in range(depth):
            for k in range(groups):
                last_ref[z, strided(k), :] = u_ref[steps - 1, own + z, k]
        for z in range(planes):
            for k in range(groups):
                whole_ref[z, k] = u_ref[steps - 1, z, k]


def chain(idx, first, rest, before=None):
    count = len(first)
    depth, nx, ny = first[0].shape
    steps = rest[0].shape[0]
    planes, groups = depth * count, nx // ROWS
    field = (planes, groups, ROWS, ny)
    quarter = jax.ShapeDtypeStruct((depth, nx, ny), jnp.float32)
    operands = [idx, *first, *rest]
    if before is None:
        outs = (quarter, jax.ShapeDtypeStruct(field, jnp.float32))
    else:
        operands.append(before)
        outs = (
            jax.ShapeDtypeStruct((steps, depth, nx, ny), jnp.float32),
            quarter,
            jax.ShapeDtypeStruct((1, ny), jnp.float32),
        )
    vmem = pl.BlockSpec(memory_space=pltpu.VMEM)
    return pl.pallas_call(
        functools.partial(chain_kernel, count, steps, before is not None),
        out_shape=outs,
        in_specs=[pl.BlockSpec(memory_space=pltpu.SMEM)] + [vmem] * (len(operands) - 1),
        out_specs=jax.tree.map(lambda _: vmem, outs),
        scratch_shapes=[pltpu.VMEM(field, jnp.float32)] * 6 + [pltpu.VMEM((steps, *field), jnp.float32)] * 2,
        name="chain" if before is None else "chain_keep",
    )(*operands)


def local(state, source, absorption):
    space, slab = lax.axis_index("space"), lax.axis_index("tm")
    has_next = (slab < lax.axis_size("tm") - 1).astype(jnp.int32)
    idx = jnp.stack([space.astype(jnp.int32), has_next])
    stacked = jnp.concatenate([source[1:], absorption[None], state[:1]], axis=0)
    gathered = pieces_of(stacked)
    rest = [g[:-1] for g in gathered]
    last, before = chain(idx, [g[-1] for g in gathered], rest)
    coarse = next_slab(last) + source[0]
    relaxed, change, partial = chain(idx, pieces_of(coarse), rest, before)
    residual = next_slab(change)
    bit = 1
    while bit < lax.axis_size("tm"):
        partial = partial + partner(partial, "tm", bit)
        bit *= 2
    return relaxed, residual[None], partial[0, 0]


def solution(mesh):
    return jax.shard_map(
        local,
        mesh=mesh,
        in_specs=(
            P("tm", "space", None, None),
            P("tm", "space", None, None),
            P("space", None, None),
        ),
        out_specs=(P("tm", "space", None, None), P("tm", "space", None, None), P()),
        check_vma=False,
    )
```

```python
import functools
import math

import jax
import jax.numpy as jnp
from jax import lax
from jax.experimental import pallas as pl
from jax.experimental.pallas import tpu as pltpu
from jax.sharding import PartitionSpec as P

SWEEPS = 5
COUPLING = 4.0
ROWS = 8
LAG = 1
VMEM_BYTES = 20 * 1024 * 1024


def sweep_weights(count):
    spread = 6.0 * COUPLING / (1.0 + 6.0 * COUPLING)
    return [
        1.0 / (1.0 + spread * math.cos(math.pi * (2 * k + 1) / (2 * count))) for k in range(count)
    ]


def step_polynomial():
    rest = [0.0, 1.0]
    for w in sweep_weights(SWEEPS):
        grown = [0.0] * (len(rest) + 1)
        for i, c in enumerate(rest):
            grown[i] += c * (1.0 - w)
            grown[i + 1] += c * w
        rest = grown
    top = [-c for c in rest]
    top[0] += 1.0
    quotient, carry = [], 0.0
    for c in top[:-1]:
        carry += c
        quotient.append(carry)
    return quotient[0], quotient[2], quotient[4]


def partner(value, axis, bit):
    count = lax.axis_size(axis)
    return lax.ppermute(value, axis, [(i, i ^ bit) for i in range(count)])


def next_slab(value):
    count = lax.axis_size("tm")
    return lax.ppermute(value, "tm", [(i, i + 1) for i in range(count - 1)])


def across(value):
    return partner(value, "space", lax.axis_size("space") // 2)


def pieces_of(value, crossed):
    count = lax.axis_size("space")
    found = {0: value, count // 2: crossed}
    bit = count // 4
    while bit:
        found.update({m ^ bit: partner(v, "space", bit) for m, v in list(found.items())})
        bit //= 2
    return [found[m] for m in range(count)]


def relax(steps, h_ref, g_ref, a_ref, b_ref, c_ref, d_ref, s_ref, write):
    planes, groups, rows, lanes = g_ref.shape
    c0, c1, c2 = (c / COUPLING for c in step_polynomial())
    row = lax.broadcasted_iota(jnp.int32, (rows, lanes), 0)
    lane = lax.broadcasted_iota(jnp.int32, (rows, lanes), 1)
    not_top, not_bottom = row != 0, row != rows - 1
    not_left, not_right = lane != 0, lane != lanes - 1

    def jacobi(f_ref, z):
        field = [f_ref[z, k] for k in range(groups)]
        above = jnp.where(not_top, pltpu.roll(field[-1], 1, 0), 0.0)
        below = jnp.where(not_bottom, pltpu.roll(field[0], rows - 1, 0), 0.0)
        for k in range(groups):
            total = (field[k - 1] if k else above) + (field[k + 1] if k < groups - 1 else below)
            if z:
                total = total + f_ref[z - 1, k]
            if z < planes - 1:
                total = total + f_ref[z + 1, k]
            left = jnp.where(not_left, pltpu.roll(field[k], 1, 1), 0.0)
            right = jnp.where(not_right, pltpu.roll(field[k], lanes - 1, 1), 0.0)
            yield k, h_ref[z, k] * (total + (left + right))

    def step(j, carry):
        def level0(z):
            for k, v in jacobi(g_ref, z):
                a_ref[z, k] = v

        def level1(z):
            for k, v in jacobi(a_ref, z):
                b_ref[z, k] = c1 * g_ref[z, k] + c2 * v

        def level2(z):
            for k, v in jacobi(b_ref, z):
                c_ref[z, k] = v

        def level3(z):
            for k, v in jacobi(c_ref, z):
                d_ref[z, k] = c0 * g_ref[z, k] + v

        def level4(z):
            for k, v in jacobi(d_ref, z):
                u = (d_ref[z, k] + v) + s_ref[j, z, k]
                write(j, z, k, u)
                g_ref[z, k] = h_ref[z, k] * u

        levels = [level0, level1, level2, level3, level4]
        for t in range(planes + LAG * (len(levels) - 1)):
            for i, level in enumerate(levels):
                z = t - LAG * i
                if 0 <= z < planes:
                    level(z)
        return carry

    lax.fori_loop(0, steps, step, 0)


def strided(k, groups):
    return pl.ds(k, ROWS, stride=groups)


def cells(idx, pieces, groups):
    for m, piece in enumerate(pieces):
        depth = piece.shape[-3]
        for z in range(depth):
            for k in range(groups):
                yield piece, z, strided(k, groups), (idx ^ m) * depth + z, k


def open_kernel(count, idx_ref, *refs):
    pieces, (h_ref, v_ref, g_ref, a_ref, b_ref, c_ref, d_ref, s_ref) = refs[:count], refs[count:]
    groups = g_ref.shape[1]
    zero = jnp.zeros(g_ref.shape[2:], jnp.float32)
    for piece, z, at, plane, k in cells(idx_ref[0], pieces, groups):
        h = COUPLING / (1.0 + 6.0 * COUPLING + piece[1, z, at, :])
        h_ref[plane, k] = h
        g_ref[plane, k] = h * piece[0, z, at, :]
        s_ref[0, plane, k] = piece[2, z, at, :]
        s_ref[1, plane, k] = zero

    def write(j, z, k, u):
        v_ref[z, k] = u

    relax(2, h_ref, g_ref, a_ref, b_ref, c_ref, d_ref, s_ref, write)


def close_kernel(count, idx_ref, h_ref, v_ref, *refs):
    pieces, (whole_ref, half_ref, g_ref, a_ref, b_ref, c_ref, d_ref, s_ref) = refs[:count], refs[count:]
    planes, groups = g_ref.shape[:2]
    steps = s_ref.shape[0]
    zero = jnp.zeros(g_ref.shape[2:], jnp.float32)
    for piece, z, at, plane, k in cells(idx_ref[0], pieces, groups):
        g_ref[plane, k] = h_ref[plane, k] * (v_ref[plane, k] + piece[0, z, at, :])
        for j in range(steps - 1):
            s_ref[j, plane, k] = piece[j + 1, z, at, :]
        s_ref[steps - 1, plane, k] = zero

    def write(j, z, k, u):
        whole_ref[z, k] = u

    relax(steps, h_ref, g_ref, a_ref, b_ref, c_ref, d_ref, s_ref, write)
    start = (idx_ref[0] & 1) * (planes // 2)
    for z in range(planes // 2):
        for k in range(groups):
            half_ref[z, k] = whole_ref[start + z, k]


def final_kernel(count, idx_ref, h_ref, before_ref, mine_ref, other_ref, *refs):
    coarse, opens, closes = refs[:count], refs[count : 2 * count], refs[2 * count : 3 * count]
    relaxed_ref, change_ref, norm_ref, g_ref, a_ref, b_ref, c_ref, d_ref, s_ref, u_ref = refs[3 * count :]
    planes, groups = g_ref.shape[:2]
    steps, depth = relaxed_ref.shape[:2]
    idx = idx_ref[0]
    zero = jnp.zeros(g_ref.shape[2:], jnp.float32)
    start = idx & 1
    for z in range(planes // 2):
        for k in range(groups):
            u_ref[0, start * (planes // 2) + z, k] = mine_ref[z, k]
            u_ref[0, (1 - start) * (planes // 2) + z, k] = other_ref[z, k]
    for piece, z, at, plane, k in cells(idx, coarse, groups):
        u = u_ref[0, plane, k] + piece[0, z, at, :]
        if piece is coarse[0]:
            relaxed_ref[0, z, at, :] = u
        g_ref[plane, k] = h_ref[plane, k] * u
    for piece, z, at, plane, k in cells(idx, opens, groups):
        s_ref[0, plane, k] = piece[2, z, at, :]
        s_ref[steps - 1, plane, k] = zero
    for piece, z, at, plane, k in cells(idx, closes, groups):
        for j in range(1, steps - 1):
            s_ref[j, plane, k] = piece[j - 1, z, at, :]

    def write(j, z, k, u):
        u_ref[j, z, k] = u

    relax(steps, h_ref, g_ref, a_ref, b_ref, c_ref, d_ref, s_ref, write)

    own = idx * depth
    partial = [zero] * groups
    for z in range(planes):
        for k in range(groups):
            change = u_ref[steps - 1, z, k] - before_ref[z, k]
            a_ref[z, k] = change
            partial[k] = partial[k] + change * change
    for z in range(depth):
        for k in range(groups):
            at = strided(k, groups)
            for j in range(steps - 1):
                relaxed_ref[j + 1, z, at, :] = u_ref[j, own + z, k]
            change_ref[z, at, :] = a_ref[own + z, k]
    partial = jnp.sum(functools.reduce(jnp.add, partial), axis=0, keepdims=True)
    total = jnp.sum(partial, axis=1, keepdims=True) * idx_ref[1].astype(jnp.float32)
    norm_ref[...] = jnp.broadcast_to(total, norm_ref.shape)


def call(kernel, name, operands, outs, scratch):
    vmem = pl.BlockSpec(memory_space=pltpu.VMEM)
    return pl.pallas_call(
        kernel,
        out_shape=tuple(jax.ShapeDtypeStruct(shape, jnp.float32) for shape in outs),
        in_specs=[pl.BlockSpec(memory_space=pltpu.SMEM)] + [vmem] * (len(operands) - 1),
        out_specs=(vmem,) * len(outs),
        scratch_shapes=[pltpu.VMEM(shape, jnp.float32) for shape in scratch],
        compiler_params=pltpu.CompilerParams(vmem_limit_bytes=VMEM_BYTES),
        name=name,
    )(*operands)


def local(state, source, absorption):
    space, slab = lax.axis_index("space"), lax.axis_index("tm")
    count, slabs = lax.axis_size("space"), lax.axis_size("tm")
    steps, depth, nx, ny = source.shape
    planes, groups = depth * count, nx // ROWS
    field = (planes, groups, ROWS, ny)
    half = (planes // 2, groups, ROWS, ny)
    has_next = (slab < slabs - 1).astype(jnp.int32)
    idx = jnp.stack([space.astype(jnp.int32), has_next])

    opens = jnp.concatenate([state[:1], absorption[None], source[1:2]], axis=0)
    closes, coarse = source[2:], source[:1]
    crossed = across(opens)
    closes_crossed = across(closes)
    coarse_crossed = across(coarse)
    opens = pieces_of(opens, crossed)

    h, v = call(
        functools.partial(open_kernel, count), "open", [idx, *opens], [field] * 2, [field] * 5 + [(2, *field)]
    )
    closes_crossed, v = lax.optimization_barrier((closes_crossed, v))
    closes = pieces_of(closes, closes_crossed)
    before, mine = call(
        functools.partial(close_kernel, count),
        "close",
        [idx, h, v, *closes],
        [field, half],
        [field] * 5 + [(steps - 2, *field)],
    )
    coarse_crossed, mine = lax.optimization_barrier((coarse_crossed, mine))
    mine = next_slab(mine)
    coarse = pieces_of(coarse, coarse_crossed)
    other = partner(mine, "space", 1)
    relaxed, change, partial = call(
        functools.partial(final_kernel, count),
        "final",
        [idx, h, before, mine, other, *coarse, *opens, *closes],
        [source.shape, (depth, nx, ny), (1, ny)],
        [field] * 5 + [(steps, *field)] * 2,
    )
    residual = next_slab(change)
    bit = 1
    while bit < slabs:
        partial = partial + partner(partial, "tm", bit)
        bit *= 2
    return relaxed, residual[None], partial[0, 0]


def solution(mesh):
    return jax.shard_map(
        local,
        mesh=mesh,
        in_specs=(
            P("tm", "space", None, None),
            P("tm", "space", None, None),
            P("space", None, None),
        ),
        out_specs=(P("tm", "space", None, None), P("tm", "space", None, None), P()),
        check_vma=False,
    )
```

```python
import functools
import math

import jax
import jax.numpy as jnp
from jax import lax
from jax.experimental import pallas as pl
from jax.experimental.pallas import tpu as pltpu
from jax.sharding import PartitionSpec as P

SWEEPS = 5
COUPLING = 4.0
ROWS = 8
LAG = 1
VMEM_BYTES = 20 * 1024 * 1024


def sweep_weights(count):
    spread = 6.0 * COUPLING / (1.0 + 6.0 * COUPLING)
    return [
        1.0 / (1.0 + spread * math.cos(math.pi * (2 * k + 1) / (2 * count))) for k in range(count)
    ]


def step_polynomial():
    rest = [0.0, 1.0]
    for w in sweep_weights(SWEEPS):
        grown = [0.0] * (len(rest) + 1)
        for i, c in enumerate(rest):
            grown[i] += c * (1.0 - w)
            grown[i + 1] += c * w
        rest = grown
    top = [-c for c in rest]
    top[0] += 1.0
    quotient, carry = [], 0.0
    for c in top[:-1]:
        carry += c
        quotient.append(carry)
    return quotient[0], quotient[2], quotient[4]


def partner(value, axis, bit):
    count = lax.axis_size(axis)
    return lax.ppermute(value, axis, [(i, i ^ bit) for i in range(count)])


def next_slab(value):
    count = lax.axis_size("tm")
    return lax.ppermute(value, "tm", [(i, i + 1) for i in range(count - 1)])


def across(value):
    return partner(value, "space", lax.axis_size("space") // 2)


def pieces_of(value, crossed):
    count = lax.axis_size("space")
    found = {0: value, count // 2: crossed}
    bit = count // 4
    while bit:
        found.update({m ^ bit: partner(v, "space", bit) for m, v in list(found.items())})
        bit //= 2
    return [found[m] for m in range(count)]


def relax(steps, h_ref, g_ref, a_ref, b_ref, c_ref, d_ref, s_ref, write):
    planes, groups, rows, lanes = g_ref.shape
    c0, c1, c2 = (c / COUPLING for c in step_polynomial())
    row = lax.broadcasted_iota(jnp.int32, (rows, lanes), 0)
    lane = lax.broadcasted_iota(jnp.int32, (rows, lanes), 1)
    not_top, not_bottom = row != 0, row != rows - 1
    not_left, not_right = lane != 0, lane != lanes - 1

    def jacobi(f_ref, z):
        field = [f_ref[z, k] for k in range(groups)]
        above = jnp.where(not_top, pltpu.roll(field[-1], 1, 0), 0.0)
        below = jnp.where(not_bottom, pltpu.roll(field[0], rows - 1, 0), 0.0)
        for k in range(groups):
            total = (field[k - 1] if k else above) + (field[k + 1] if k < groups - 1 else below)
            if z:
                total = total + f_ref[z - 1, k]
            if z < planes - 1:
                total = total + f_ref[z + 1, k]
            left = jnp.where(not_left, pltpu.roll(field[k], 1, 1), 0.0)
            right = jnp.where(not_right, pltpu.roll(field[k], lanes - 1, 1), 0.0)
            yield k, h_ref[z, k] * (total + (left + right))

    def step(j, carry):
        def level0(z):
            for k, v in jacobi(g_ref, z):
                a_ref[z, k] = v

        def level1(z):
            for k, v in jacobi(a_ref, z):
                b_ref[z, k] = c1 * g_ref[z, k] + c2 * v

        def level2(z):
            for k, v in jacobi(b_ref, z):
                c_ref[z, k] = v

        def level3(z):
            for k, v in jacobi(c_ref, z):
                d_ref[z, k] = c0 * g_ref[z, k] + v

        def level4(z):
            for k, v in jacobi(d_ref, z):
                u = (d_ref[z, k] + v) + s_ref[j, z, k]
                write(j, z, k, u)
                g_ref[z, k] = h_ref[z, k] * u

        levels = [level0, level1, level2, level3, level4]
        for t in range(planes + LAG * (len(levels) - 1)):
            for i, level in enumerate(levels):
                z = t - LAG * i
                if 0 <= z < planes:
                    level(z)
        return carry

    lax.fori_loop(0, steps, step, 0)


def strided(k, groups):
    return pl.ds(k, ROWS, stride=groups)


def cells(idx, pieces, groups):
    for m, piece in enumerate(pieces):
        depth = piece.shape[-3]
        for z in range(depth):
            for k in range(groups):
                yield piece, z, strided(k, groups), (idx ^ m) * depth + z, k


def open_kernel(count, idx_ref, *refs):
    pieces, (h_ref, v_ref, g_ref, a_ref, b_ref, c_ref, d_ref, s_ref) = refs[:count], refs[count:]
    groups = g_ref.shape[1]
    zero = jnp.zeros(g_ref.shape[2:], jnp.float32)
    for piece, z, at, plane, k in cells(idx_ref[0], pieces, groups):
        h = COUPLING / (1.0 + 6.0 * COUPLING + piece[1, z, at, :])
        h_ref[plane, k] = h
        g_ref[plane, k] = h * piece[0, z, at, :]
        s_ref[0, plane, k] = piece[2, z, at, :]
        s_ref[1, plane, k] = zero

    def write(j, z, k, u):
        v_ref[z, k] = u

    relax(2, h_ref, g_ref, a_ref, b_ref, c_ref, d_ref, s_ref, write)


def close_kernel(count, idx_ref, h_ref, v_ref, *refs):
    pieces, (whole_ref, half_ref, g_ref, a_ref, b_ref, c_ref, d_ref, s_ref) = refs[:count], refs[count:]
    planes, groups = g_ref.shape[:2]
    steps = s_ref.shape[0]
    zero = jnp.zeros(g_ref.shape[2:], jnp.float32)
    for piece, z, at, plane, k in cells(idx_ref[0], pieces, groups):
        g_ref[plane, k] = h_ref[plane, k] * (v_ref[plane, k] + piece[0, z, at, :])
        for j in range(steps - 1):
            s_ref[j, plane, k] = piece[j + 1, z, at, :]
        s_ref[steps - 1, plane, k] = zero

    def write(j, z, k, u):
        whole_ref[z, k] = u

    relax(steps, h_ref, g_ref, a_ref, b_ref, c_ref, d_ref, s_ref, write)
    start = (idx_ref[0] & 1) * (planes // 2)
    for z in range(planes // 2):
        for k in range(groups):
            half_ref[z, k] = whole_ref[start + z, k]


def sort_kernel(count, idx_ref, *refs):
    coarse, opens, closes = refs[:count], refs[count : 2 * count], refs[2 * count : 3 * count]
    s_ref = refs[3 * count]
    groups = s_ref.shape[2]
    steps = s_ref.shape[0] - 1
    zero = jnp.zeros(s_ref.shape[3:], jnp.float32)
    for piece, z, at, plane, k in cells(idx_ref[0], coarse, groups):
        s_ref[steps, plane, k] = piece[0, z, at, :]
        s_ref[steps - 1, plane, k] = zero
    for piece, z, at, plane, k in cells(idx_ref[0], opens, groups):
        s_ref[0, plane, k] = piece[2, z, at, :]
    for piece, z, at, plane, k in cells(idx_ref[0], closes, groups):
        for j in range(1, steps - 1):
            s_ref[j, plane, k] = piece[j - 1, z, at, :]


def final_kernel(idx_ref, h_ref, before_ref, s_ref, mine_ref, other_ref, *refs):
    relaxed_ref, change_ref, norm_ref, g_ref, a_ref, b_ref, c_ref, d_ref, u_ref = refs
    planes, groups = g_ref.shape[:2]
    steps, depth = relaxed_ref.shape[:2]
    idx = idx_ref[0]
    zero = jnp.zeros(g_ref.shape[2:], jnp.float32)
    for part, received in (((idx & 1), mine_ref), (1 - (idx & 1), other_ref)):
        for z in range(planes // 2):
            plane = part * (planes // 2) + z
            for k in range(groups):
                u = received[z, k] + s_ref[steps, plane, k]
                a_ref[plane, k] = u
                g_ref[plane, k] = h_ref[plane, k] * u
    for z in range(depth):
        for k in range(groups):
            relaxed_ref[0, z, strided(k, groups), :] = a_ref[idx * depth + z, k]

    def write(j, z, k, u):
        u_ref[j, z, k] = u

    relax(steps, h_ref, g_ref, a_ref, b_ref, c_ref, d_ref, s_ref, write)

    own = idx * depth
    partial = [zero] * groups
    for z in range(planes):
        for k in range(groups):
            change = u_ref[steps - 1, z, k] - before_ref[z, k]
            a_ref[z, k] = change
            partial[k] = partial[k] + change * change
    for z in range(depth):
        for k in range(groups):
            at = strided(k, groups)
            for j in range(steps - 1):
                relaxed_ref[j + 1, z, at, :] = u_ref[j, own + z, k]
            change_ref[z, at, :] = a_ref[own + z, k]
    partial = jnp.sum(functools.reduce(jnp.add, partial), axis=0, keepdims=True)
    total = jnp.sum(partial, axis=1, keepdims=True) * idx_ref[1].astype(jnp.float32)
    norm_ref[...] = jnp.broadcast_to(total, norm_ref.shape)


def call(kernel, operands, outs, scratch):
    vmem = pl.BlockSpec(memory_space=pltpu.VMEM)
    return pl.pallas_call(
        kernel,
        out_shape=tuple(jax.ShapeDtypeStruct(shape, jnp.float32) for shape in outs),
        in_specs=[pl.BlockSpec(memory_space=pltpu.SMEM)] + [vmem] * (len(operands) - 1),
        out_specs=(vmem,) * len(outs),
        scratch_shapes=[pltpu.VMEM(shape, jnp.float32) for shape in scratch],
        compiler_params=pltpu.CompilerParams(vmem_limit_bytes=VMEM_BYTES),
    )(*operands)


def relaxation(state, source, absorption):
    space, slab = lax.axis_index("space"), lax.axis_index("tm")
    count, slabs = lax.axis_size("space"), lax.axis_size("tm")
    steps, depth, nx, ny = source.shape
    planes, groups = depth * count, nx // ROWS
    field = (planes, groups, ROWS, ny)
    half = (planes // 2, groups, ROWS, ny)
    has_next = (slab < slabs - 1).astype(jnp.int32)
    idx = jnp.stack([space.astype(jnp.int32), has_next])

    opens = jnp.concatenate([state[:1], absorption[None], source[1:2]], axis=0)
    closes, coarse = source[2:], source[:1]
    crossed = across(opens)
    closes_crossed = across(closes)
    coarse_crossed = across(coarse)
    opens = pieces_of(opens, crossed)

    h, v = call(functools.partial(open_kernel, count), [idx, *opens], [field] * 2, [field] * 5 + [(2, *field)])
    closes_crossed, v = lax.optimization_barrier((closes_crossed, v))
    closes = pieces_of(closes, closes_crossed)
    before, mine = call(
        functools.partial(close_kernel, count), [idx, h, v, *closes], [field, half], [field] * 5 + [(steps - 2, *field)]
    )
    coarse_crossed, before = lax.optimization_barrier((coarse_crossed, before))
    coarse = pieces_of(coarse, coarse_crossed)
    mine = next_slab(mine)
    (sources,) = call(functools.partial(sort_kernel, count), [idx, *coarse, *opens, *closes], [(steps + 1, *field)], [])
    mine, sources = lax.optimization_barrier((mine, sources))
    other = partner(mine, "space", 1)
    relaxed, change, partial = call(
        final_kernel,
        [idx, h, before, sources, mine, other],
        [source.shape, (depth, nx, ny), (1, ny)],
        [field] * 5 + [(steps, *field)],
    )
    residual = next_slab(change)
    bit = 1
    while bit < slabs:
        if 2 * bit >= slabs:
            residual, partial = lax.optimization_barrier((residual, partial))
        partial = partial + partner(partial, "tm", bit)
        bit *= 2
    return relaxed, residual[None], partial[0, 0]


def solution(mesh):
    return jax.shard_map(
        relaxation,
        mesh=mesh,
        in_specs=(
            P("tm", "space", None, None),
            P("tm", "space", None, None),
            P("space", None, None),
        ),
        out_specs=(P("tm", "space", None, None), P("tm", "space", None, None), P()),
        check_vma=False,
    )
```
